16 devices in a mesh: rep: 2 (over y, z), dp: 8 (over x, core).
Axes of the slice: x: 4, y: 2, z: 1, core: 2. Of those that a mesh axis runs over, the one named last changes fastest.
The devices are a block of a 4x4x8 slice.
Arguments:
- a: bfloat16 [16, 4, 4096, 1024], P(('rep', 'dp')), parts along dimension 0
- g: bfloat16 [16, 4, 4096, 2816], P(('rep', 'dp')), parts along dimension 0
Outputs:
- output: bfloat16 [8, 1024, 2816], P('rep'), parts along dimension 0
There are 2 independent parts. The reference program is written for one: setup_inputs(seed, part) draws one part's arguments, and reference() takes and returns one part's arrays. A program takes and returns all parts, laid end to end along the dimension named above; each array names one.
All inputs are finite; a program needn't handle non-finite values.
Results may differ from the reference program's by a relative error of at most 0.012.
Values are sent between devices in bfloat16 or wider.
A program may use at most 768 MiB of HBM per device.

```python
import jax
import jax.numpy as jnp
from jax import lax

DEVICES = 8
MATRICES = 4
TOKENS = 4096
D = 1024
FF = 2816


def setup_inputs(seed: int = 0, part: int = 0) -> dict:
    ka, kg, ks = (jax.random.fold_in(k, part) for k in jax.random.split(jax.random.key(seed), 3))
    size = 2.0 ** jax.random.uniform(ks, (DEVICES, MATRICES, 1, 1), jnp.float32, -1.0, 1.0)
    a = jax.random.normal(ka, (DEVICES, MATRICES, TOKENS, D), jnp.float32)
    g = size * jax.random.normal(kg, (DEVICES, MATRICES, TOKENS, FF), jnp.float32) * (DEVICES * TOKENS) ** -0.5
    return {"a": a.astype(jnp.bfloat16), "g": g.astype(jnp.bfloat16)}


def reference(a, g):
    def take(so_far, one):
        return so_far + jnp.einsum("ntd,ntf->ndf", *one, preferred_element_type=jnp.float32), None

    return lax.scan(take, jnp.zeros((MATRICES, D, FF), jnp.float32), (a, g))[0].astype(jnp.bfloat16)
```

```python
import functools

import jax
import jax.numpy as jnp
from jax import lax
from jax.experimental import pallas as pl
from jax.experimental.pallas import tpu as pltpu
from jax.sharding import PartitionSpec as P

MESH = pl.DeviceIdType.MESH
WIDTH = 256
CORES = 2
LAG = (1, 3, 5)
EVERY = 4
FORWARD, LAST = 3, 6
SLOTS = 8
SWAPS = 4
DEEP = 3
F32 = jnp.float32
CONTRACT = (((0,), (0,)), ((), ()))


def kernel(chips, a_hbm, g_hbm, out, a_buf, g_buf, acc, own, swap, sends, lands,
           a_sem, g_sem, swap_send, swap_recv, send_sem, recv_sem, hop_send, gather_recv, across_send, across_recv):
    matrices = a_hbm.shape[1]
    chunks, rows, width = out.shape
    per = chunks // matrices
    half = rows // CORES
    block = half // chips
    kept = own.shape[0]

    rep, me = lax.axis_index("rep"), lax.axis_index("dp")
    chip, core = me // CORES, lax.rem(me, CORES)
    sign = 1 - 2 * core
    ahead = lax.rem(chip + sign + chips, chips)
    behind = lax.rem(chip - sign + chips, chips)
    opposite = lax.rem(chip + 2, chips)
    to_ahead, to_behind = (rep, ahead * CORES + core), (rep, behind * CORES + core)
    to_other = (rep, chip * CORES + 1 - core)

    barrier = pltpu.get_barrier_semaphore()
    for device in (to_ahead, to_behind, to_other):
        pl.semaphore_signal(barrier, inc=1, device_id=device, device_id_type=MESH)
    pl.semaphore_wait(barrier, 3)

    def remote(src, dst, send, recv, device):
        return pltpu.make_async_remote_copy(
            src_ref=src, dst_ref=dst, send_sem=send, recv_sem=recv, device_id=device, device_id_type=MESH
        )

    def a_copy(n):
        slot = lax.rem(n, 2)
        return pltpu.make_async_copy(a_hbm.at[0, n], a_buf.at[slot], a_sem.at[slot])

    def g_copy(u):
        slot = lax.rem(u, DEEP)
        columns = pl.ds(pl.multiple_of(lax.rem(u, per) * width, width), width)
        return pltpu.make_async_copy(g_hbm.at[0, u // per, :, columns], g_buf.at[slot], g_sem.at[slot])

    def in_half(b):
        return pl.ds(pl.multiple_of(b * block, block), block)

    def in_chunk(b):
        return pl.ds(pl.multiple_of(core * half + b * block, block), block)

    mine = pl.ds(pl.multiple_of(core * half, half), half)
    others = pl.ds(pl.multiple_of((1 - core) * half, half), half)

    def swap_copy(u):
        slot = lax.rem(u, SWAPS)
        return remote(swap.at[slot], out.at[u, others], swap_send.at[slot], swap_recv.at[u], to_other)

    def reduce_copy(kind, u, device):
        slot = lax.rem(u, SLOTS)
        return remote(sends.at[kind, slot], lands.at[kind, u], send_sem.at[kind, slot], recv_sem.at[kind, u], device)

    first = functools.partial(reduce_copy, 0, device=to_ahead)
    second = functools.partial(reduce_copy, 1, device=to_ahead)
    direct = functools.partial(reduce_copy, 2, device=to_behind)

    def gather_copy(kind, u, b, device):
        piece = out.at[u, in_chunk(b)]
        return remote(piece, piece, hop_send, gather_recv.at[kind, u], device)

    def across(u, b):
        piece = out.at[u, in_chunk(b)]
        return remote(piece, piece, across_send, across_recv, to_other)

    def multiply(u):
        n = u // per
        slot = lax.rem(u, DEEP)

        @pl.when(lax.rem(u, per) == 0)
        def _():
            a_copy(n).wait()

            @pl.when(n + 1 < matrices)
            def _():
                a_copy(n + 1).start()

        @pl.when(u + DEEP - 1 < chunks)
        def _():
            g_copy(u + DEEP - 1).start()

        g_copy(u).wait()
        acc[...] = lax.dot_general(a_buf[lax.rem(n, 2)], g_buf[slot], CONTRACT, preferred_element_type=F32)

        @pl.when(u >= SWAPS)
        def _():
            swap_copy(u - SWAPS).wait_send()

        swap[lax.rem(u, SWAPS)] = acc[others, :].astype(swap.dtype)
        swap_copy(u).start()
        own[lax.rem(u, kept)] = acc[mine, :]

    def of_chip(u, b):
        return own[lax.rem(u, kept), in_half(b), :] + out[u, in_chunk(b), :].astype(F32)

    def put(kind, u, value):
        sends[kind, lax.rem(u, SLOTS)] = value.astype(sends.dtype)

    def free(copy, u):
        @pl.when(u >= SLOTS)
        def _():
            copy(u - SLOTS).wait_send()

    def stage_1(u):
        swap_copy(u).wait_recv()
        free(first, u)
        put(0, u, of_chip(u, opposite))
        first(u).start()
        free(direct, u)
        put(2, u, of_chip(u, behind))
        direct(u).start()

    def stage_2(u):
        first(u).wait_recv()
        free(second, u)
        put(1, u, of_chip(u, ahead) + lands[0, u].astype(F32))
        second(u).start()

    def stage_3(u):
        second(u).wait_recv()
        direct(u).wait_recv()
        total = of_chip(u, chip) + lands[1, u].astype(F32) + lands[2, u].astype(F32)
        out[u, in_chunk(chip), :] = total.astype(out.dtype)

    stages = (stage_1, stage_2, stage_3)

    def gather(k):
        @pl.when(k < chunks)
        def _():
            gather_copy(0, k, chip, to_ahead).start()
            gather_copy(1, k, chip, to_behind).start()
            across(k, chip).start()

        @pl.when((k >= FORWARD) & (k < chunks + FORWARD))
        def _():
            u = k - FORWARD
            gather_copy(0, u, behind, to_ahead).wait_recv()
            gather_copy(2, u, behind, to_ahead).start()
            across(u, behind).start()
            gather_copy(1, u, ahead, to_behind).wait_recv()
            across(u, ahead).start()

        @pl.when((k >= LAST) & (k < chunks + LAST))
        def _():
            u = k - LAST
            gather_copy(2, u, opposite, to_ahead).wait_recv()
            across(u, opposite).start()

    a_copy(0).start()
    for u in range(DEEP - 1):
        g_copy(u).start()

    begin = LAG[-1] + 1
    early = (chunks - begin + EVERY - 1) // EVERY

    @pl.loop(0, chunks)
    def _(s):
        multiply(s)
        for stage, lag in zip(stages, LAG):
            pl.when(s >= lag)(functools.partial(stage, s - lag))
        pl.when((s >= begin) & (lax.rem(s - begin, EVERY) == 0))(lambda: gather((s - begin) // EVERY))

    @pl.loop(0, LAG[-1])
    def _(t):
        for stage, lag in zip(stages, LAG):
            pl.when(t < lag)(functools.partial(stage, t + chunks - lag))
        gather(t + early)

    @pl.loop(early + LAG[-1], chunks + LAST)
    def _(k):
        gather(k)

    @pl.loop(chunks - SLOTS, chunks)
    def _(u):
        for copy in (first, second, direct):
            copy(u).wait_send()

    @pl.loop(chunks - SWAPS, chunks)
    def _(u):
        swap_copy(u).wait_send()

    three = out.at[:, pl.ds(0, 3 * block)]
    remote(three, three, hop_send, across_recv, to_ahead).wait_send()
    remote(out.at[:, mine], out.at[:, others], across_send, across_recv, to_other).wait()


def place(per, sums, out, sem):
    chunks, _, width = sums.shape

    def copy(u):
        columns = pl.ds(pl.multiple_of(lax.rem(u, per) * width, width), width)
        return pltpu.make_async_copy(sums.at[u], out.at[u // per, :, columns], sem.at[u])

    @pl.loop(0, chunks)
    def _(u):
        copy(u).start()

    @pl.loop(0, chunks)
    def _(u):
        copy(u).wait()


def solution(mesh):
    chips = mesh.shape["dp"] // CORES

    def step(a, g):
        _, matrices, tokens, rows = a.shape
        columns = g.shape[3]
        width, dtype = WIDTH, a.dtype
        per = columns // width
        chunks = matrices * per
        half = rows // CORES
        block = half // chips
        flops = 2 * matrices * tokens * rows * columns
        sems = pltpu.SemaphoreType.DMA
        sums = pl.pallas_call(
            functools.partial(kernel, chips),
            name="multiply_and_sum",
            out_shape=pltpu.VMEM((chunks, rows, width), dtype),
            in_specs=[pl.BlockSpec(memory_space=pl.ANY)] * 2,
            out_specs=pl.BlockSpec(memory_space=pltpu.VMEM),
            scratch_shapes=[
                pltpu.VMEM((2, tokens, rows), dtype),
                pltpu.VMEM((DEEP, tokens, width), dtype),
                pltpu.VMEM((rows, width), F32),
                pltpu.VMEM((LAG[-1] + 1, half, width), F32),
                pltpu.VMEM((SWAPS, half, width), dtype),
                pltpu.VMEM((3, SLOTS, block, width), dtype),
                pltpu.VMEM((3, chunks, block, width), dtype),
                sems((2,)),
                sems((DEEP,)),
                sems((SWAPS,)),
                sems((chunks,)),
                sems((3, SLOTS)),
                sems((3, chunks)),
                sems,
                sems((3, chunks)),
                sems,
                sems,
            ],
            compiler_params=pltpu.CompilerParams(
                collective_id=0, has_side_effects=True, vmem_limit_bytes=40 * 2**20
            ),
            cost_estimate=pl.CostEstimate(flops=flops, bytes_accessed=2 * (a.size + g.size), transcendentals=0),
        )(a, g)
        return pl.pallas_call(
            functools.partial(place, per),
            name="place",
            out_shape=jax.ShapeDtypeStruct((matrices, rows, columns), dtype),
            in_specs=[pl.BlockSpec(memory_space=pltpu.VMEM)],
            out_specs=pl.BlockSpec(memory_space=pl.ANY),
            scratch_shapes=[sems((chunks,))],
            compiler_params=pltpu.CompilerParams(vmem_limit_bytes=2**20),
        )(sums)

    return jax.shard_map(
        step,
        mesh=mesh,
        in_specs=(P(("rep", "dp")), P(("rep", "dp"))),
        out_specs=P("rep"),
        check_vma=False,
    )
```

```python
import functools

import jax
import jax.numpy as jnp
from jax import lax
from jax.experimental import pallas as pl
from jax.experimental.pallas import tpu as pltpu
from jax.sharding import PartitionSpec as P

MESH = pl.DeviceIdType.MESH
WIDTH = 256
CORES = 2
HALVED, TURN = 4, 8
FIRST, SECOND, THIRD = ((0, 0), (HALVED, 1)), ((0, 1), (HALVED, 2), (TURN, 3)), ((0, 2), (HALVED, 3), (TURN, 5))
EVERY = 2
FORWARD, LAST = 3, 6
TURNS = 12
PARTS = 4
SLOTS = 8
SWAPS = 4
DEEP = 3
F32 = jnp.float32
CONTRACT = (((0,), (0,)), ((), ()))


def late(s, lag, limit):
    due, u = False, 0
    for (n, steps), end in zip(lag, [n for n, _ in lag[1:]] + [limit]):
        here = (s - steps >= n) & (s - steps < end)
        due, u = due | here, jnp.where(here, s - steps, u)
    return due, u


def kernel(chips, a_hbm, g_hbm, out, a_buf, g_buf, acc, own, swap, sends, lands,
           part_sem, a_sem, g_sem, swap_send, swap_recv, send_sem, recv_sem, hop_send, gather_recv, across_send, across_recv):
    matrices = a_hbm.shape[1]
    chunks, rows, width = out.shape
    per = chunks // matrices
    half = rows // CORES
    block = half // chips
    kept = own.shape[0]
    depth = a_buf.shape[1] // PARTS

    rep, me = lax.axis_index("rep"), lax.axis_index("dp")
    chip, core = me // CORES, lax.rem(me, CORES)
    sign = 1 - 2 * core
    ahead = lax.rem(chip + sign + chips, chips)
    behind = lax.rem(chip - sign + chips, chips)
    opposite = lax.rem(chip + 2, chips)
    to_ahead, to_behind = (rep, ahead * CORES + core), (rep, behind * CORES + core)
    to_other = (rep, chip * CORES + 1 - core)

    barrier = pltpu.get_barrier_semaphore()
    for device in (to_ahead, to_behind, to_other):
        pl.semaphore_signal(barrier, inc=1, device_id=device, device_id_type=MESH)

    def remote(src, dst, send, recv, device):
        return pltpu.make_async_remote_copy(
            src_ref=src, dst_ref=dst, send_sem=send, recv_sem=recv, device_id=device, device_id_type=MESH
        )

    def a_copy(n):
        slot = lax.rem(n, 2)
        return pltpu.make_async_copy(a_hbm.at[0, n], a_buf.at[slot], a_sem.at[slot])

    def g_copy(u):
        slot = lax.rem(u, DEEP)
        columns = pl.ds(pl.multiple_of(lax.rem(u, per) * width, width), width)
        return pltpu.make_async_copy(g_hbm.at[0, u // per, :, columns], g_buf.at[slot], g_sem.at[slot])

    def in_half(b):
        return pl.ds(pl.multiple_of(b * block, block), block)

    def in_chunk(b):
        return pl.ds(pl.multiple_of(core * half + b * block, block), block)

    mine = pl.ds(pl.multiple_of(core * half, half), half)
    others = pl.ds(pl.multiple_of((1 - core) * half, half), half)

    def swap_copy(u):
        slot = lax.rem(u, SWAPS)
        return remote(swap.at[slot], out.at[u, others], swap_send.at[slot], swap_recv.at[lax.rem(u, TURNS)], to_other)

    def reduce_copy(kind, u, device):
        slot = lax.rem(u, SLOTS)
        return remote(sends.at[kind, slot], lands.at[kind, u], send_sem.at[kind, slot], recv_sem.at[kind, lax.rem(u, TURNS)], device)

    first = functools.partial(reduce_copy, 0, device=to_ahead)
    second = functools.partial(reduce_copy, 1, device=to_ahead)
    direct = functools.partial(reduce_copy, 2, device=to_behind)

    def gather_copy(kind, u, b, device):
        piece = out.at[u, in_chunk(b)]
        return remote(piece, piece, hop_send, gather_recv.at[kind, lax.rem(u, TURNS)], device)

    def across(u, b):
        piece = out.at[u, in_chunk(b)]
        return remote(piece, piece, across_send, across_recv, to_other)

    def dot(a, g):
        return lax.dot_general(a, g, CONTRACT, preferred_element_type=F32)

    def quarters(h):
        part = half // 2
        for q in range(2):
            yield pl.ds(q * part, part), pl.ds(pl.multiple_of(h * half + q * part, part), part)

    def multiply(u, halved):
        n = u // per

        @pl.when(lax.rem(u, per) == 0)
        def _():
            a_copy(n).wait()

        @pl.when((lax.rem(u, per) == 1) & (n + 1 < matrices))
        def _():
            a_copy(n + 1).start()

        @pl.when(u + DEEP - 1 < chunks)
        def _():
            g_copy(u + DEEP - 1).start()

        @pl.when(u >= SWAPS)
        def _():
            swap_copy(u - SWAPS).wait_send()

        g_copy(u).wait()
        if halved:
            for to, at in quarters(1 - core):
                value = dot(a_buf[lax.rem(n, 2), :, at], g_buf[lax.rem(u, DEEP)])
                swap[lax.rem(u, SWAPS), to] = value.astype(swap.dtype)
            swap_copy(u).start()
            for to, at in quarters(core):
                own[lax.rem(u, kept), to] = dot(a_buf[lax.rem(n, 2), :, at], g_buf[lax.rem(u, DEEP)])
            return

        for c in range(CORES):

            @pl.when(core == c)
            def _():
                value = dot(a_buf[lax.rem(n, 2)], g_buf[lax.rem(u, DEEP)])
                halves = [value[h * half : (h + 1) * half] for h in range(CORES)]
                swap[lax.rem(u, SWAPS)] = halves[1 - c].astype(swap.dtype)
                own[lax.rem(u, kept)] = halves[c]

        swap_copy(u).start()

    def part_copy(kind, p):
        tokens = pl.ds(p * depth, depth)
        if kind == 2:
            columns = pl.ds(0, width)
            return pltpu.make_async_copy(g_hbm.at[0, 0, tokens, columns], g_buf.at[0, tokens], part_sem.at[kind, p])
        columns = mine if kind else others
        return pltpu.make_async_copy(
            a_hbm.at[0, 0, tokens, columns], a_buf.at[0, tokens, columns], part_sem.at[kind, p]
        )

    def multiply_first():
        for p in range(PARTS):
            tokens = pl.ds(p * depth, depth)
            part_copy(0, p).wait()
            part_copy(2, p).wait()
            for to, at in quarters(1 - core):
                value = dot(a_buf[0, tokens, at], g_buf[0, tokens])
                acc[to] = acc[to] + value if p else value
        swap[0] = acc[...].astype(swap.dtype)
        pl.semaphore_wait(barrier, 3)
        swap_copy(0).start()
        for p in range(PARTS):
            tokens = pl.ds(p * depth, depth)
            part_copy(1, p).wait()
            for to, at in quarters(core):
                value = dot(a_buf[0, tokens, at], g_buf[0, tokens])
                own[0, to] = own[0, to] + value if p else value

    def of_chip(u, b):
        return own[lax.rem(u, kept), in_half(b), :] + out[u, in_chunk(b), :].astype(F32)

    def put(kind, u, value):
        sends[kind, lax.rem(u, SLOTS)] = value.astype(sends.dtype)

    def free(copy, u):
        @pl.when(u >= SLOTS)
        def _():
            copy(u - SLOTS).wait_send()

    def stage_1(u):
        swap_copy(u).wait_recv()
        free(first, u)
        put(0, u, of_chip(u, opposite))
        first(u).start()
        free(direct, u)
        put(2, u, of_chip(u, behind))
        direct(u).start()

    def stage_2(u):
        first(u).wait_recv()
        free(second, u)
        put(1, u, of_chip(u, ahead) + lands[0, u].astype(F32))
        second(u).start()

    def stage_3(u):
        second(u).wait_recv()
        direct(u).wait_recv()
        total = of_chip(u, chip) + lands[1, u].astype(F32) + lands[2, u].astype(F32)
        out[u, in_chunk(chip), :] = total.astype(out.dtype)

    def when(due, act):
        pl.when(due[0])(lambda: act(due[1]))

    def gather(k):
        @pl.when(k < chunks)
        def _():
            gather_copy(0, k, chip, to_ahead).start()
            gather_copy(1, k, chip, to_behind).start()
            across(k, chip).start()

        @pl.when((k >= FORWARD) & (k < chunks + FORWARD))
        def _():
            u = k - FORWARD
            gather_copy(0, u, behind, to_ahead).wait_recv()
            gather_copy(2, u, behind, to_ahead).start()
            across(u, behind).start()
            gather_copy(1, u, ahead, to_behind).wait_recv()
            across(u, ahead).start()

        @pl.when((k >= LAST) & (k < chunks + LAST))
        def _():
            u = k - LAST
            gather_copy(2, u, opposite, to_ahead).wait_recv()
            across(u, opposite).start()

    for p in range(PARTS):
        part_copy(2, p).start()
        part_copy(0, p).start()
    for p in range(PARTS):
        part_copy(1, p).start()
    for u in range(1, DEEP):
        g_copy(u).start()
    multiply_first()
    stage_1(0)

    later = THIRD[-1][1]
    settled = TURN + later
    early = TURN + (chunks - settled + EVERY - 1) // EVERY

    def reduce(s):
        when(late(s, FIRST, chunks), stage_1)
        when(late(s, SECOND, chunks), stage_2)
        when(late(s, THIRD, chunks), stage_3)

    def step(s, halved):
        multiply(s, halved)
        reduce(s)
        due, k = late(s, THIRD[:-1], TURN)
        after = s >= settled
        due = due | (after & (lax.rem(s - settled, EVERY) == 0))
        when((due, jnp.where(after, TURN + (s - settled) // EVERY, k)), gather)

    pl.loop(1, HALVED)(functools.partial(step, halved=True))
    pl.loop(HALVED, chunks)(functools.partial(step, halved=False))

    @pl.loop(0, later)
    def _(t):
        reduce(t + chunks)
        gather(t + early)

    @pl.loop(early + later, chunks + LAST)
    def _(k):
        gather(k)

    @pl.loop(chunks - SLOTS, chunks)
    def _(u):
        for copy in (first, second, direct):
            copy(u).wait_send()

    @pl.loop(chunks - SWAPS, chunks)
    def _(u):
        swap_copy(u).wait_send()

    three = out.at[:, pl.ds(0, 3 * block)]
    remote(three, three, hop_send, across_recv, to_ahead).wait_send()
    remote(out.at[:, mine], out.at[:, others], across_send, across_recv, to_other).wait()


def place(per, sums, out, sem):
    chunks, _, width = sums.shape

    def copy(u):
        columns = pl.ds(pl.multiple_of(lax.rem(u, per) * width, width), width)
        return pltpu.make_async_copy(sums.at[u], out.at[u // per, :, columns], sem.at[u])

    @pl.loop(0, chunks)
    def _(u):
        copy(u).start()

    @pl.loop(0, chunks)
    def _(u):
        copy(u).wait()


def solution(mesh):
    chips = mesh.shape["dp"] // CORES

    def step(a, g):
        _, matrices, tokens, rows = a.shape
        columns = g.shape[3]
        width, dtype = WIDTH, a.dtype
        per = columns // width
        chunks = matrices * per
        half = rows // CORES
        block = half // chips
        flops = 2 * matrices * tokens * rows * columns
        sems = pltpu.SemaphoreType.DMA
        sums = pl.pallas_call(
            functools.partial(kernel, chips),
            name="multiply_and_sum",
            out_shape=pltpu.VMEM((chunks, rows, width), dtype),
            in_specs=[pl.BlockSpec(memory_space=pl.ANY)] * 2,
            out_specs=pl.BlockSpec(memory_space=pltpu.VMEM),
            scratch_shapes=[
                pltpu.VMEM((2, tokens, rows), dtype),
                pltpu.VMEM((DEEP, tokens, width), dtype),
                pltpu.VMEM((half, width), F32),
                pltpu.VMEM((THIRD[-1][1] + 1, half, width), F32),
                pltpu.VMEM((SWAPS, half, width), dtype),
                pltpu.VMEM((3, SLOTS, block, width), dtype),
                pltpu.VMEM((3, chunks, block, width), dtype),
                sems((3, PARTS)),
                sems((2,)),
                sems((DEEP,)),
                sems((SWAPS,)),
                sems((TURNS,)),
                sems((3, SLOTS)),
                sems((3, TURNS)),
                sems,
                sems((3, TURNS)),
                sems,
                sems,
            ],
            compiler_params=pltpu.CompilerParams(
                collective_id=0, has_side_effects=True, vmem_limit_bytes=40 * 2**20
            ),
            cost_estimate=pl.CostEstimate(flops=flops, bytes_accessed=2 * (a.size + g.size), transcendentals=0),
        )(a, g)
        return pl.pallas_call(
            functools.partial(place, per),
            name="place",
            out_shape=jax.ShapeDtypeStruct((matrices, rows, columns), dtype),
            in_specs=[pl.BlockSpec(memory_space=pltpu.VMEM)],
            out_specs=pl.BlockSpec(memory_space=pl.ANY),
            scratch_shapes=[sems((chunks,))],
            compiler_params=pltpu.CompilerParams(vmem_limit_bytes=2**20),
        )(sums)

    return jax.shard_map(
        step,
        mesh=mesh,
        in_specs=(P(("rep", "dp")), P(("rep", "dp"))),
        out_specs=P("rep"),
        check_vma=False,
    )
```

```python
import functools

import jax
import jax.numpy as jnp
from jax import lax
from jax.experimental import pallas as pl
from jax.experimental.pallas import tpu as pltpu
from jax.sharding import PartitionSpec as P

MESH = pl.DeviceIdType.MESH
WIDTH = 256
CORES = 2
SECOND, THIRD = ((0, 1), (8, 2)), ((0, 3), (8, 4))
TURN = 12
EVERY = 2
FORWARD, LAST = 3, 6
TURNS = 10
PARTS = 4
SLOTS = 6
SWAPS = 4
DEEP = 3
F32 = jnp.float32
CONTRACT = (((0,), (0,)), ((), ()))


def late(s, lag, limit):
    due, u = False, 0
    for (n, steps), end in zip(lag, [n for n, _ in lag[1:]] + [limit]):
        here = (s - steps >= n) & (s - steps < end)
        due, u = due | here, jnp.where(here, s - steps, u)
    return due, u


def kernel(chips, a_hbm, g_hbm, out, a_buf, g_buf, acc, own, swap, sends, lands,
           part_sem, a_sem, g_sem, swap_send, swap_recv, send_sem, recv_sem, hop_send, gather_recv, across_send, across_recv):
    matrices = a_hbm.shape[1]
    chunks, rows, width = out.shape
    per = chunks // matrices
    half = rows // CORES
    block = half // chips
    kept = own.shape[0]
    depth = a_buf.shape[1] // PARTS

    rep, me = lax.axis_index("rep"), lax.axis_index("dp")
    chip, core = me // CORES, lax.rem(me, CORES)
    sign = 1 - 2 * core
    ahead = lax.rem(chip + sign + chips, chips)
    behind = lax.rem(chip - sign + chips, chips)
    opposite = lax.rem(chip + 2, chips)
    to_ahead, to_behind = (rep, ahead * CORES + core), (rep, behind * CORES + core)
    to_other = (rep, chip * CORES + 1 - core)

    barrier = pltpu.get_barrier_semaphore()
    for device in (to_ahead, to_behind, to_other):
        pl.semaphore_signal(barrier, inc=1, device_id=device, device_id_type=MESH)

    def remote(src, dst, send, recv, device):
        return pltpu.make_async_remote_copy(
            src_ref=src, dst_ref=dst, send_sem=send, recv_sem=recv, device_id=device, device_id_type=MESH
        )

    def a_copy(n):
        slot = lax.rem(n, 2)
        return pltpu.make_async_copy(a_hbm.at[0, n], a_buf.at[slot], a_sem.at[slot])

    def g_copy(u):
        slot = lax.rem(u, DEEP)
        columns = pl.ds(pl.multiple_of(lax.rem(u, per) * width, width), width)
        return pltpu.make_async_copy(g_hbm.at[0, u // per, :, columns], g_buf.at[slot], g_sem.at[slot])

    def in_half(b):
        return pl.ds(pl.multiple_of(b * block, block), block)

    def in_chunk(b):
        return pl.ds(pl.multiple_of(core * half + b * block, block), block)

    mine = pl.ds(pl.multiple_of(core * half, half), half)
    others = pl.ds(pl.multiple_of((1 - core) * half, half), half)

    def swap_copy(u):
        slot = lax.rem(u, SWAPS)
        return remote(swap.at[slot], out.at[u, others], swap_send.at[slot], swap_recv.at[lax.rem(u, TURNS)], to_other)

    def reduce_copy(kind, u, device):
        slot = lax.rem(u, SLOTS)
        return remote(sends.at[kind, slot], lands.at[kind, u], send_sem.at[kind, slot], recv_sem.at[kind, lax.rem(u, TURNS)], device)

    first = functools.partial(reduce_copy, 0, device=to_ahead)
    second = functools.partial(reduce_copy, 1, device=to_ahead)
    direct = functools.partial(reduce_copy, 2, device=to_behind)

    def gather_copy(kind, u, b, device):
        piece = out.at[u, in_chunk(b)]
        return remote(piece, piece, hop_send, gather_recv.at[kind, lax.rem(u, TURNS)], device)

    def across(u, b):
        piece = out.at[u, in_chunk(b)]
        return remote(piece, piece, across_send, across_recv, to_other)

    def dot(a, g):
        return lax.dot_general(a, g, CONTRACT, preferred_element_type=F32)

    def quarters(h):
        part = half // 2
        for q in range(2):
            yield pl.ds(q * part, part), pl.ds(pl.multiple_of(h * half + q * part, part), part)

    def multiply(u):
        n = u // per

        @pl.when(lax.rem(u, per) == 0)
        def _():
            a_copy(n).wait()

        @pl.when((lax.rem(u, per) == 1) & (n + 1 < matrices))
        def _():
            a_copy(n + 1).start()

        @pl.when(u + DEEP - 1 < chunks)
        def _():
            g_copy(u + DEEP - 1).start()

        @pl.when(u >= SWAPS)
        def _():
            swap_copy(u - SWAPS).wait_send()

        g_copy(u).wait()
        for to, at in quarters(1 - core):
            value = dot(a_buf[lax.rem(n, 2), :, at], g_buf[lax.rem(u, DEEP)])
            swap[lax.rem(u, SWAPS), to] = value.astype(swap.dtype)
        swap_copy(u).start()
        for to, at in quarters(core):
            own[lax.rem(u, kept), to] = dot(a_buf[lax.rem(n, 2), :, at], g_buf[lax.rem(u, DEEP)])

    def part_copy(kind, p):
        tokens = pl.ds(p * depth, depth)
        if kind == 2:
            columns = pl.ds(0, width)
            return pltpu.make_async_copy(g_hbm.at[0, 0, tokens, columns], g_buf.at[0, tokens], part_sem.at[kind, p])
        columns = mine if kind else others
        return pltpu.make_async_copy(
            a_hbm.at[0, 0, tokens, columns], a_buf.at[0, tokens, columns], part_sem.at[kind, p]
        )

    def multiply_first():
        for p in range(PARTS):
            tokens = pl.ds(p * depth, depth)
            part_copy(0, p).wait()
            part_copy(2, p).wait()
            for to, at in quarters(1 - core):
                value = dot(a_buf[0, tokens, at], g_buf[0, tokens])
                acc[to] = acc[to] + value if p else value
        swap[0] = acc[...].astype(swap.dtype)
        pl.semaphore_wait(barrier, 3)
        swap_copy(0).start()
        for p in range(PARTS):
            tokens = pl.ds(p * depth, depth)
            part_copy(1, p).wait()
            for to, at in quarters(core):
                value = dot(a_buf[0, tokens, at], g_buf[0, tokens])
                own[0, to] = own[0, to] + value if p else value

    def of_chip(u, b):
        return own[lax.rem(u, kept), in_half(b), :] + out[u, in_chunk(b), :].astype(F32)

    def put(kind, u, value):
        sends[kind, lax.rem(u, SLOTS)] = value.astype(sends.dtype)

    def free(copy, u):
        @pl.when(u >= SLOTS)
        def _():
            copy(u - SLOTS).wait_send()

    def stage_1(u):
        swap_copy(u).wait_recv()
        free(first, u)
        put(0, u, of_chip(u, opposite))
        first(u).start()
        free(direct, u)
        put(2, u, of_chip(u, behind))
        direct(u).start()

    def stage_2(u):
        first(u).wait_recv()
        free(second, u)
        put(1, u, of_chip(u, ahead) + lands[0, u].astype(F32))
        second(u).start()

    def stage_3(u):
        second(u).wait_recv()
        direct(u).wait_recv()
        total = of_chip(u, chip) + lands[1, u].astype(F32) + lands[2, u].astype(F32)
        out[u, in_chunk(chip), :] = total.astype(out.dtype)

    def when(due, act):
        pl.when(due[0])(lambda: act(due[1]))

    def gather(k):
        @pl.when(k < chunks)
        def _():
            gather_copy(0, k, chip, to_ahead).start()
            gather_copy(1, k, chip, to_behind).start()
            across(k, chip).start()

        @pl.when((k >= FORWARD) & (k < chunks + FORWARD))
        def _():
            u = k - FORWARD
            gather_copy(0, u, behind, to_ahead).wait_recv()
            gather_copy(2, u, behind, to_ahead).start()
            across(u, behind).start()
            gather_copy(1, u, ahead, to_behind).wait_recv()
            across(u, ahead).start()

        @pl.when((k >= LAST) & (k < chunks + LAST))
        def _():
            u = k - LAST
            gather_copy(2, u, opposite, to_ahead).wait_recv()
            across(u, opposite).start()

    for p in range(PARTS):
        part_copy(2, p).start()
        part_copy(0, p).start()
    for p in range(PARTS):
        part_copy(1, p).start()
    for u in range(1, DEEP):
        g_copy(u).start()
    multiply_first()
    stage_1(0)

    later = THIRD[-1][1]
    settled = TURN + later
    early = TURN + (chunks - settled + EVERY - 1) // EVERY

    def reduce(s):
        pl.when(s < chunks)(lambda: stage_1(s))
        when(late(s, SECOND, chunks), stage_2)
        when(late(s, THIRD, chunks), stage_3)

    @pl.loop(1, chunks)
    def _(s):
        multiply(s)
        reduce(s)
        due, k = late(s, THIRD, TURN)
        after = s >= settled
        due = due | (after & (lax.rem(s - settled, EVERY) == 0))
        when((due, jnp.where(after, TURN + (s - settled) // EVERY, k)), gather)

    @pl.loop(0, later)
    def _(t):
        reduce(t + chunks)
        gather(t + early)

    @pl.loop(early + later, chunks + LAST)
    def _(k):
        gather(k)

    @pl.loop(chunks - SLOTS, chunks)
    def _(u):
        for copy in (first, second, direct):
            copy(u).wait_send()

    @pl.loop(chunks - SWAPS, chunks)
    def _(u):
        swap_copy(u).wait_send()

    three = out.at[:, pl.ds(0, 3 * block)]
    remote(three, three, hop_send, across_recv, to_ahead).wait_send()
    remote(out.at[:, mine], out.at[:, others], across_send, across_recv, to_other).wait()


def place(per, sums, out, sem):
    chunks, _, width = sums.shape

    def copy(u):
        columns = pl.ds(pl.multiple_of(lax.rem(u, per) * width, width), width)
        return pltpu.make_async_copy(sums.at[u], out.at[u // per, :, columns], sem.at[u])

    @pl.loop(0, chunks)
    def _(u):
        copy(u).start()

    @pl.loop(0, chunks)
    def _(u):
        copy(u).wait()


def solution(mesh):
    chips = mesh.shape["dp"] // CORES

    def step(a, g):
        _, matrices, tokens, rows = a.shape
        columns = g.shape[3]
        width, dtype = WIDTH, a.dtype
        per = columns // width
        chunks = matrices * per
        half = rows // CORES
        block = half // chips
        flops = 2 * matrices * tokens * rows * columns
        sems = pltpu.SemaphoreType.DMA
        sums = pl.pallas_call(
            functools.partial(kernel, chips),
            name="multiply_and_sum",
            out_shape=pltpu.VMEM((chunks, rows, width), dtype),
            in_specs=[pl.BlockSpec(memory_space=pl.ANY)] * 2,
            out_specs=pl.BlockSpec(memory_space=pltpu.VMEM),
            scratch_shapes=[
                pltpu.VMEM((2, tokens, rows), dtype),
                pltpu.VMEM((DEEP, tokens, width), dtype),
                pltpu.VMEM((half, width), F32),
                pltpu.VMEM((THIRD[-1][1] + 1, half, width), F32),
                pltpu.VMEM((SWAPS, half, width), dtype),
                pltpu.VMEM((3, SLOTS, block, width), dtype),
                pltpu.VMEM((3, chunks, block, width), dtype),
                sems((3, PARTS)),
                sems((2,)),
                sems((DEEP,)),
                sems((SWAPS,)),
                sems((TURNS,)),
                sems((3, SLOTS)),
                sems((3, TURNS)),
                sems,
                sems((3, TURNS)),
                sems,
                sems,
            ],
            compiler_params=pltpu.CompilerParams(
                collective_id=0, has_side_effects=True, vmem_limit_bytes=40 * 2**20
            ),
            cost_estimate=pl.CostEstimate(flops=flops, bytes_accessed=2 * (a.size + g.size), transcendentals=0),
        )(a, g)
        return pl.pallas_call(
            functools.partial(place, per),
            name="place",
            out_shape=jax.ShapeDtypeStruct((matrices, rows, columns), dtype),
            in_specs=[pl.BlockSpec(memory_space=pltpu.VMEM)],
            out_specs=pl.BlockSpec(memory_space=pl.ANY),
            scratch_shapes=[sems((chunks,))],
            compiler_params=pltpu.CompilerParams(vmem_limit_bytes=2**20),
        )(sums)

    return jax.shard_map(
        step,
        mesh=mesh,
        in_specs=(P(("rep", "dp")), P(("rep", "dp"))),
        out_specs=P("rep"),
        check_vma=False,
    )
```

```python
import functools

import jax
import jax.numpy as jnp
from jax import lax
from jax.experimental import pallas as pl
from jax.experimental.pallas import tpu as pltpu
from jax.sharding import PartitionSpec as P

MESH = pl.DeviceIdType.MESH
WIDTH = 256
CORES = 2
SECOND, THIRD = ((0, 1), (8, 2)), ((0, 3), (8, 5))
TURN = 12
EVERY = 2
FORWARD, LAST = 3, 6
TURNS = 10
PARTS = 4
SLOTS = 6
SWAPS = 4
DEEP = 3
F32 = jnp.float32
CONTRACT = (((0,), (0,)), ((), ()))


def late(s, lag, limit):
    due, u = False, 0
    for (n, steps), end in zip(lag, [n for n, _ in lag[1:]] + [limit]):
        here = (s - steps >= n) & (s - steps < end)
        due, u = due | here, jnp.where(here, s - steps, u)
    return due, u


def kernel(chips, a_hbm, g_hbm, out, a_buf, g_buf, acc, own, swap, sends, lands,
           part_sem, a_sem, g_sem, swap_send, swap_recv, send_sem, recv_sem, hop_send, gather_recv, across_send, across_recv):
    matrices = a_hbm.shape[1]
    chunks, rows, width = out.shape
    per = chunks // matrices
    half = rows // CORES
    block = half // chips
    kept = own.shape[0]
    depth = a_buf.shape[1] // PARTS

    rep, me = lax.axis_index("rep"), lax.axis_index("dp")
    chip, core = me // CORES, lax.rem(me, CORES)
    sign = 1 - 2 * core
    ahead = lax.rem(chip + sign + chips, chips)
    behind = lax.rem(chip - sign + chips, chips)
    opposite = lax.rem(chip + 2, chips)
    to_ahead, to_behind = (rep, ahead * CORES + core), (rep, behind * CORES + core)
    to_other = (rep, chip * CORES + 1 - core)

    barrier = pltpu.get_barrier_semaphore()
    for device in (to_ahead, to_behind, to_other):
        pl.semaphore_signal(barrier, inc=1, device_id=device, device_id_type=MESH)

    def remote(src, dst, send, recv, device):
        return pltpu.make_async_remote_copy(
            src_ref=src, dst_ref=dst, send_sem=send, recv_sem=recv, device_id=device, device_id_type=MESH
        )

    def a_copy(n):
        slot = lax.rem(n, 2)
        return pltpu.make_async_copy(a_hbm.at[0, n], a_buf.at[slot], a_sem.at[slot])

    def g_copy(u):
        slot = lax.rem(u, DEEP)
        columns = pl.ds(pl.multiple_of(lax.rem(u, per) * width, width), width)
        return pltpu.make_async_copy(g_hbm.at[0, u // per, :, columns], g_buf.at[slot], g_sem.at[slot])

    def in_half(b):
        return pl.ds(pl.multiple_of(b * block, block), block)

    def in_chunk(b):
        return pl.ds(pl.multiple_of(core * half + b * block, block), block)

    mine = pl.ds(pl.multiple_of(core * half, half), half)
    others = pl.ds(pl.multiple_of((1 - core) * half, half), half)

    def swap_copy(u):
        slot = lax.rem(u, SWAPS)
        return remote(swap.at[slot], out.at[u, others], swap_send.at[slot], swap_recv.at[lax.rem(u, TURNS)], to_other)

    def reduce_copy(kind, u, device):
        slot = lax.rem(u, SLOTS)
        return remote(sends.at[kind, slot], lands.at[kind, u], send_sem.at[kind, slot], recv_sem.at[kind, lax.rem(u, TURNS)], device)

    first = functools.partial(reduce_copy, 0, device=to_ahead)
    second = functools.partial(reduce_copy, 1, device=to_ahead)
    direct = functools.partial(reduce_copy, 2, device=to_behind)

    def gather_copy(kind, u, b, device):
        piece = out.at[u, in_chunk(b)]
        return remote(piece, piece, hop_send, gather_recv.at[kind, lax.rem(u, TURNS)], device)

    def across(u, b):
        piece = out.at[u, in_chunk(b)]
        return remote(piece, piece, across_send, across_recv, to_other)

    def dot(a, g):
        return lax.dot_general(a, g, CONTRACT, preferred_element_type=F32)

    def quarters(h):
        part = half // 2
        for q in range(2):
            yield pl.ds(q * part, part), pl.ds(pl.multiple_of(h * half + q * part, part), part)

    def multiply(u, between):
        n = u // per

        @pl.when(lax.rem(u, per) == 0)
        def _():
            a_copy(n).wait()

        @pl.when((lax.rem(u, per) == 1) & (n + 1 < matrices))
        def _():
            a_copy(n + 1).start()

        @pl.when(u + DEEP - 1 < chunks)
        def _():
            g_copy(u + DEEP - 1).start()

        @pl.when(u >= SWAPS)
        def _():
            swap_copy(u - SWAPS).wait_send()

        g_copy(u).wait()
        for to, at in quarters(1 - core):
            value = dot(a_buf[lax.rem(n, 2), :, at], g_buf[lax.rem(u, DEEP)])
            swap[lax.rem(u, SWAPS), to] = value.astype(swap.dtype)
        swap_copy(u).start()
        between()
        for to, at in quarters(core):
            own[lax.rem(u, kept), to] = dot(a_buf[lax.rem(n, 2), :, at], g_buf[lax.rem(u, DEEP)])

    def part_copy(kind, p):
        tokens = pl.ds(p * depth, depth)
        if kind == 2:
            columns = pl.ds(0, width)
            return pltpu.make_async_copy(g_hbm.at[0, 0, tokens, columns], g_buf.at[0, tokens], part_sem.at[kind, p])
        columns = mine if kind else others
        return pltpu.make_async_copy(
            a_hbm.at[0, 0, tokens, columns], a_buf.at[0, tokens, columns], part_sem.at[kind, p]
        )

    def multiply_first():
        for p in range(PARTS):
            tokens = pl.ds(p * depth, depth)
            part_copy(0, p).wait()
            part_copy(2, p).wait()
            for to, at in quarters(1 - core):
                value = dot(a_buf[0, tokens, at], g_buf[0, tokens])
                acc[to] = acc[to] + value if p else value
        swap[0] = acc[...].astype(swap.dtype)
        pl.semaphore_wait(barrier, 3)
        swap_copy(0).start()
        for p in range(PARTS):
            tokens = pl.ds(p * depth, depth)
            part_copy(1, p).wait()
            for to, at in quarters(core):
                value = dot(a_buf[0, tokens, at], g_buf[0, tokens])
                own[0, to] = own[0, to] + value if p else value

    def of_chip(u, b):
        return own[lax.rem(u, kept), in_half(b), :] + out[u, in_chunk(b), :].astype(F32)

    def put(kind, u, value):
        sends[kind, lax.rem(u, SLOTS)] = value.astype(sends.dtype)

    def free(copy, u):
        @pl.when(u >= SLOTS)
        def _():
            copy(u - SLOTS).wait_send()

    def stage_1(u):
        swap_copy(u).wait_recv()
        free(first, u)
        put(0, u, of_chip(u, opposite))
        first(u).start()
        free(direct, u)
        put(2, u, of_chip(u, behind))
        direct(u).start()

    def stage_2(u):
        first(u).wait_recv()
        free(second, u)
        put(1, u, of_chip(u, ahead) + lands[0, u].astype(F32))
        second(u).start()

    def stage_3(u):
        second(u).wait_recv()
        direct(u).wait_recv()
        total = of_chip(u, chip) + lands[1, u].astype(F32) + lands[2, u].astype(F32)
        out[u, in_chunk(chip), :] = total.astype(out.dtype)

    def when(due, act):
        pl.when(due[0])(lambda: act(due[1]))

    def gather(k):
        @pl.when(k < chunks)
        def _():
            gather_copy(0, k, chip, to_ahead).start()
            gather_copy(1, k, chip, to_behind).start()
            across(k, chip).start()

        @pl.when((k >= FORWARD) & (k < chunks + FORWARD))
        def _():
            u = k - FORWARD
            gather_copy(0, u, behind, to_ahead).wait_recv()
            gather_copy(2, u, behind, to_ahead).start()
            across(u, behind).start()
            gather_copy(1, u, ahead, to_behind).wait_recv()
            across(u, ahead).start()

        @pl.when((k >= LAST) & (k < chunks + LAST))
        def _():
            u = k - LAST
            gather_copy(2, u, opposite, to_ahead).wait_recv()
            across(u, opposite).start()

    for p in range(PARTS):
        part_copy(2, p).start()
        part_copy(0, p).start()
    for p in range(PARTS):
        part_copy(1, p).start()
    for u in range(1, DEEP):
        g_copy(u).start()
    multiply_first()
    stage_1(0)

    later = THIRD[-1][1]
    settled = TURN + later
    early = TURN + (chunks - settled + EVERY - 1) // EVERY

    def reduce(s):
        pl.when(s < chunks)(lambda: stage_1(s))
        when(late(s, SECOND, chunks), stage_2)

    def finish(s):
        when(late(s, THIRD, chunks), stage_3)

    def between(s):
        finish(s)
        due, k = late(s, THIRD, TURN)
        after = s >= settled
        due = due | (after & (lax.rem(s - settled, EVERY) == 0))
        when((due, jnp.where(after, TURN + (s - settled) // EVERY, k)), gather)

    @pl.loop(1, chunks)
    def _(s):
        multiply(s, functools.partial(between, s))
        reduce(s)

    @pl.loop(0, later)
    def _(t):
        finish(t + chunks)
        reduce(t + chunks)
        gather(t + early)

    @pl.loop(early + later, chunks + LAST)
    def _(k):
        gather(k)

    @pl.loop(chunks - SLOTS, chunks)
    def _(u):
        for copy in (first, second, direct):
            copy(u).wait_send()

    @pl.loop(chunks - SWAPS, chunks)
    def _(u):
        swap_copy(u).wait_send()

    three = out.at[:, pl.ds(0, 3 * block)]
    remote(three, three, hop_send, across_recv, to_ahead).wait_send()
    remote(out.at[:, mine], out.at[:, others], across_send, across_recv, to_other).wait()


def place(per, sums, out, sem):
    chunks, _, width = sums.shape

    def copy(u):
        columns = pl.ds(pl.multiple_of(lax.rem(u, per) * width, width), width)
        return pltpu.make_async_copy(sums.at[u], out.at[u // per, :, columns], sem.at[u])

    @pl.loop(0, chunks)
    def _(u):
        copy(u).start()

    @pl.loop(0, chunks)
    def _(u):
        copy(u).wait()


def solution(mesh):
    chips = mesh.shape["dp"] // CORES

    def step(a, g):
        _, matrices, tokens, rows = a.shape
        columns = g.shape[3]
        width, dtype = WIDTH, a.dtype
        per = columns // width
        chunks = matrices * per
        half = rows // CORES
        block = half // chips
        flops = 2 * matrices * tokens * rows * columns
        sems = pltpu.SemaphoreType.DMA
        sums = pl.pallas_call(
            functools.partial(kernel, chips),
            name="multiply_and_sum",
            out_shape=pltpu.VMEM((chunks, rows, width), dtype),
            in_specs=[pl.BlockSpec(memory_space=pl.ANY)] * 2,
            out_specs=pl.BlockSpec(memory_space=pltpu.VMEM),
            scratch_shapes=[
                pltpu.VMEM((2, tokens, rows), dtype),
                pltpu.VMEM((DEEP, tokens, width), dtype),
                pltpu.VMEM((half, width), F32),
                pltpu.VMEM((THIRD[-1][1] + 1, half, width), F32),
                pltpu.VMEM((SWAPS, half, width), dtype),
                pltpu.VMEM((3, SLOTS, block, width), dtype),
                pltpu.VMEM((3, chunks, block, width), dtype),
                sems((3, PARTS)),
                sems((2,)),
                sems((DEEP,)),
                sems((SWAPS,)),
                sems((TURNS,)),
                sems((3, SLOTS)),
                sems((3, TURNS)),
                sems,
                sems((3, TURNS)),
                sems,
                sems,
            ],
            compiler_params=pltpu.CompilerParams(
                collective_id=0, has_side_effects=True, vmem_limit_bytes=40 * 2**20
            ),
            cost_estimate=pl.CostEstimate(flops=flops, bytes_accessed=2 * (a.size + g.size), transcendentals=0),
        )(a, g)
        return pl.pallas_call(
            functools.partial(place, per),
            name="place",
            out_shape=jax.ShapeDtypeStruct((matrices, rows, columns), dtype),
            in_specs=[pl.BlockSpec(memory_space=pltpu.VMEM)],
            out_specs=pl.BlockSpec(memory_space=pl.ANY),
            scratch_shapes=[sems((chunks,))],
            compiler_params=pltpu.CompilerParams(vmem_limit_bytes=2**20),
        )(sums)

    return jax.shard_map(
        step,
        mesh=mesh,
        in_specs=(P(("rep", "dp")), P(("rep", "dp"))),
        out_specs=P("rep"),
        check_vma=False,
    )
```
